256 devices in a mesh: groups: 4 (over y, x), tile: 64 (over z, core).
Axes of the slice: x: 2, y: 2, z: 32, core: 2. Of those that a mesh axis runs over, the one named last changes fastest.
The devices are a block of a 4x8x32 slice.
Arguments:
- self_query: bfloat16 [32768, 4096], P(('groups', 'tile')), parts along dimension 0, may hold values from -110 to 110
- self_key: bfloat16 [32768, 4096], P(('groups', 'tile')), parts along dimension 0, may hold values from -6 to 6
- self_value: bfloat16 [32768, 4096], P(('groups', 'tile')), parts along dimension 0, may hold values from -24 to 24
- cross_query: bfloat16 [32768, 4096], P(('groups', 'tile')), parts along dimension 0, may hold values from -110 to 110
- text_key: bfloat16 [1024, 4096], P(('groups', 'tile')), parts along dimension 0, may hold values from -6 to 6
- text_value: bfloat16 [1024, 4096], P(('groups', 'tile')), parts along dimension 0, may hold values from -24 to 24
- timestep: int32 [1], replicated, may hold values from 0 to 49
- gate_table: bfloat16 [50, 4096], replicated, may hold values from 0.5 to 2
Outputs:
- mixed: bfloat16 [32768, 4096], P(('groups', 'tile')), parts along dimension 0
The draws below stay inside these ranges and needn't reach their ends.
There are 4 independent parts, one for each index of `groups`. The reference program is written for one: setup_inputs(seed, part) draws one part's arguments, and reference() takes and returns one part's arrays. A program takes and returns all parts, laid end to end along the dimension named above; an argument that names none is the same for every part. Nothing has to cross between parts.
All inputs are finite; a program needn't handle non-finite values.
Results may differ from the reference program's by a relative error of at most 0.0032.
Values may be sent and summed in bfloat16 or wider, within the bound.
No kernel may reach another device: no remote copies, remote signals or barrier semaphores. Data moves between devices by JAX's collectives and lax.ppermute only.
A program may use at most 64 MiB of HBM per device.

```python
import math
import jax
import jax.numpy as jnp
from jax import lax

HEADS = 32
HEAD_DIM = 128
WIDTH = 4096
TOK_DEV = 128
RADIUS = 2
TEXT = 256
STEPS = 50
TILES = 64
TOKENS = 8192


def paired_draw(key, label, query_count, key_count):
    folded = jax.random.fold_in(key, label)
    width = HEADS * HEAD_DIM
    key_draw = 1.5 * jax.random.truncated_normal(jax.random.fold_in(folded, 1), -4.0, 4.0, (key_count, width), jnp.float32)
    query_draw = 1.5 * jax.random.truncated_normal(jax.random.fold_in(folded, 2), -4.0, 4.0, (query_count, width), jnp.float32)
    return (query_draw, key_draw)


def draw_self_query(key, part):
    return paired_draw(key, 11, TOKENS, TOKENS)[0].astype(jnp.bfloat16)


def draw_self_key(key, part):
    return paired_draw(key, 11, TOKENS, TOKENS)[1].astype(jnp.bfloat16)


def draw_cross_query(key, part):
    return paired_draw(key, 23, TOKENS, TEXT)[0].astype(jnp.bfloat16)


def draw_text_key(key, part):
    return paired_draw(key, 23, TOKENS, TEXT)[1].astype(jnp.bfloat16)


def steps_of(own_key, extent, pieces, smallest, high):
    factor_of, own = 1.0, jax.random.fold_in(own_key, 6)
    for dim, parts in pieces:
        steps = jnp.exp(jax.random.uniform(jax.random.fold_in(own, dim), (parts,), jnp.float32, smallest / len(pieces), high / len(pieces)))
        factor_of = factor_of * jnp.repeat(steps, extent[dim] // parts).reshape([-1 if axis == dim else 1 for axis in range(len(extent))])
    return factor_of


def noise(own_key, extent, scale, limit, pieces=(), kind=jnp.bfloat16):
    array = jax.random.normal(own_key, extent, jnp.float32) * scale
    if len(pieces) > 0:
        array = steps_of(own_key, extent, pieces, -0.22, 0.18) * array
    return jnp.clip(array, min=-limit, max=limit).astype(kind)


def setup_inputs(seed: int = 0, part: int = 0) -> dict:
    key_of = jax.random.split(jax.random.key(seed), 9)
    part_keys = jax.random.split(jax.random.fold_in(key_of[8], part), 9)
    self_query = draw_self_query(jax.random.fold_in(jax.random.fold_in(key_of[8], part), 71), part)
    self_key = draw_self_key(jax.random.fold_in(jax.random.fold_in(key_of[8], part), 71), part)
    self_value = noise(part_keys[2], (TOKENS, WIDTH), 4.0, 24.0, ((0, 64),))
    cross_query = draw_cross_query(jax.random.fold_in(jax.random.fold_in(key_of[8], part), 71), part)
    text_key = draw_text_key(jax.random.fold_in(jax.random.fold_in(key_of[8], part), 71), part)
    text_value = noise(part_keys[5], (TEXT, WIDTH), 4.0, 24.0, ((0, 64),))
    timestep = jax.random.randint(key_of[6], (1,), 0, STEPS).astype(jnp.int32)
    gate_table = jnp.clip(jax.random.uniform(key_of[7], (STEPS, WIDTH), jnp.float32, 0.5, 2.0), 0.5, 2.0).astype(jnp.bfloat16)
    return dict(self_query=self_query, self_key=self_key, self_value=self_value, cross_query=cross_query, text_key=text_key, text_value=text_value, timestep=timestep, gate_table=gate_table)


def window_attention(queries, key_block, value_block, usable):
    score_scale = 1.0 / math.sqrt(HEAD_DIM)
    scores = jnp.einsum('qhd,khd->hqk', queries, key_block) * score_scale
    masked = jnp.where(usable[None, None, :], scores, -1e+30)
    maxima = lax.optimization_barrier(jnp.max(masked, axis=2, keepdims=True))
    weights = jnp.where(usable[None, None, :], jnp.exp(masked - maxima), 0.0)
    totals = lax.optimization_barrier(jnp.sum(weights, axis=2, keepdims=True))
    rounded = lax.optimization_barrier(weights.astype(jnp.bfloat16)).astype(jnp.float32)
    summed = jnp.einsum('hqk,khd->qhd', rounded, value_block)
    return summed / jnp.transpose(totals, (1, 0, 2))

def reference(self_query, self_key, self_value, cross_query, text_key, text_value, timestep, gate_table):
    width = HEADS * HEAD_DIM
    window_span = 2 * RADIUS + 1
    margin = jnp.zeros((RADIUS * TOK_DEV, width), jnp.bfloat16)
    padded_keys = jnp.concatenate([margin, self_key, margin], axis=0)
    padded_values = jnp.concatenate([margin, self_value, margin], axis=0)
    text_keys = text_key.astype(jnp.float32).reshape(TEXT, HEADS, HEAD_DIM)
    text_values = text_value.astype(jnp.float32).reshape(TEXT, HEADS, HEAD_DIM)
    text_usable = jnp.ones((TEXT,), dtype=bool)
    gate_row = lax.dynamic_slice_in_dim(gate_table, timestep[0].astype(jnp.int32), 1, 0).astype(jnp.float32)

    def one_tile(tile_index):
        start = (tile_index * TOK_DEV).astype(jnp.int32)
        queries = lax.dynamic_slice_in_dim(self_query, start, TOK_DEV, 0).astype(jnp.float32).reshape(TOK_DEV, HEADS, HEAD_DIM)
        key_block = lax.dynamic_slice_in_dim(padded_keys, start, window_span * TOK_DEV, 0).astype(jnp.float32).reshape(window_span * TOK_DEV, HEADS, HEAD_DIM)
        value_block = lax.dynamic_slice_in_dim(padded_values, start, window_span * TOK_DEV, 0).astype(jnp.float32).reshape(window_span * TOK_DEV, HEADS, HEAD_DIM)
        offsets = jnp.arange(window_span, dtype=jnp.int32) - RADIUS
        position = tile_index + offsets
        tile_usable = (position >= 0) & (position < TILES)
        usable = jnp.repeat(tile_usable, TOK_DEV)
        self_out = window_attention(queries, key_block, value_block, usable).reshape(TOK_DEV, width)
        cross_rows = lax.dynamic_slice_in_dim(cross_query, start, TOK_DEV, 0).astype(jnp.float32).reshape(TOK_DEV, HEADS, HEAD_DIM)
        cross_out = window_attention(cross_rows, text_keys, text_values, text_usable).reshape(TOK_DEV, width)
        return (gate_row * self_out + cross_out).astype(jnp.bfloat16)
    mixed = lax.map(one_tile, jnp.arange(TILES, dtype=jnp.int32))
    return mixed.reshape(TOKENS, width)
```

```python
import math

import jax
import jax.numpy as jnp
from jax import lax
from jax.experimental import pallas as pl
from jax.experimental.pallas import tpu as pltpu
from jax.sharding import PartitionSpec as P

HEADS = 32
LOG2E = 1.4426950408889634
FEATURES = 512


def scores_of(queries, keys):
    return lax.dot_general(
        queries, keys, (((1,), (1,)), ((), ())), preferred_element_type=jnp.float32
    )


def self_kernel(bias_ref, gate_ref, query_ref, *refs, head_dim):
    key_refs, value_refs, out_ref = refs[:5], refs[5:10], refs[10]
    scale = LOG2E / math.sqrt(head_dim)
    for head in range(query_ref.shape[1] // head_dim):
        cols = slice(head * head_dim, (head + 1) * head_dim)
        queries = query_ref[:, cols]
        scores = [scores_of(queries, ref[:, cols]) for ref in key_refs]
        scores = [scores[0], scores[1]] + [
            scores[k] + bias_ref[k - 2] for k in range(2, 5)
        ]
        top = scores[0]
        for part in scores[1:]:
            top = jnp.maximum(top, part)
        top = jnp.max(top, axis=1, keepdims=True) * scale
        weights = [jnp.exp2(part * scale - top) for part in scores]
        total = weights[0]
        for part in weights[1:]:
            total = total + part
        total = jnp.sum(total, axis=1, keepdims=True)
        summed = None
        for part, ref in zip(weights, value_refs):
            product = jnp.dot(
                part.astype(jnp.bfloat16), ref[:, cols], preferred_element_type=jnp.float32
            )
            summed = product if summed is None else summed + product
        out_ref[:, cols] = summed * (1.0 / total) * gate_ref[:, cols]


def cross_kernel(core_ref, query_ref, self_ref, *refs, head_dim):
    mine, theirs, out_ref = refs[:8], refs[8:16], refs[16]
    key_buf, value_buf = refs[17], refs[18]
    rows = mine[0].shape[0]
    part = rows // 4

    def fill(keys, values):
        for k in range(8):
            key_buf[k * rows : (k + 1) * rows, :] = keys[k][...]
        for k in range(7):
            value_buf[k * rows : (k + 1) * rows, :] = values[k][...]
        for to, source in enumerate((1, 3, 0, 2)):
            first = 7 * rows + to * part
            value_buf[first : first + part, :] = values[7][source * part : (source + 1) * part, :]

    @pl.when(core_ref[0] == 0)
    def _():
        fill(mine, theirs)

    @pl.when(core_ref[0] != 0)
    def _():
        fill(theirs, mine)

    scale = LOG2E / math.sqrt(head_dim)
    for head in range(query_ref.shape[1] // head_dim):
        cols = slice(head * head_dim, (head + 1) * head_dim)
        scores = scores_of(query_ref[:, cols], key_buf[:, cols])
        top = jnp.max(scores, axis=1, keepdims=True) * scale
        weights = jnp.exp2(scores * scale - top)
        total = jnp.sum(weights, axis=1, keepdims=True)
        summed = jnp.dot(
            weights.astype(jnp.bfloat16), value_buf[:, cols], preferred_element_type=jnp.float32
        )
        out_ref[:, cols] = (self_ref[:, cols] + summed * (1.0 / total)).astype(out_ref.dtype)


def self_attention(bias, gate_row, queries, keys, values):
    rows, width = queries.shape
    block = pl.BlockSpec((rows, FEATURES), lambda i: (0, i))
    return pl.pallas_call(
        lambda *refs: self_kernel(*refs, head_dim=width // HEADS),
        grid=(width // FEATURES,),
        in_specs=[
            pl.BlockSpec(memory_space=pltpu.SMEM),
            pl.BlockSpec((1, FEATURES), lambda i: (0, i)),
        ]
        + [block] * 11,
        out_specs=block,
        out_shape=jax.ShapeDtypeStruct((rows, width), jnp.float32),
        name="self_attention",
    )(bias, gate_row, queries, *keys, *values)


def cross_attention(core, queries, self_part, mine, theirs):
    rows, width = queries.shape
    text_rows = sum(piece.shape[0] for piece in mine)
    block = pl.BlockSpec((rows, FEATURES), lambda i: (0, i))
    piece_block = pl.BlockSpec((mine[0].shape[0], FEATURES), lambda i: (0, i))
    return pl.pallas_call(
        lambda *refs: cross_kernel(*refs, head_dim=width // HEADS),
        grid=(width // FEATURES,),
        in_specs=[pl.BlockSpec(memory_space=pltpu.SMEM), block, block] + [piece_block] * 16,
        out_specs=block,
        out_shape=jax.ShapeDtypeStruct((rows, width), queries.dtype),
        scratch_shapes=[pltpu.VMEM((text_rows, FEATURES), queries.dtype)] * 2,
        name="cross_attention",
    )(core, queries, self_part, *mine, *theirs)


def shards(
    self_query, self_key, self_value, cross_query, text_key, text_value, timestep, gate_table
):
    tiles = lax.axis_size("tile")
    chips = tiles // 2
    stride = chips // 4
    place = lax.axis_index("tile")
    core = place % 2

    def from_chip(block, distance):
        return lax.ppermute(
            block, "tile", [(i, (i + 2 * distance) % tiles) for i in range(tiles)]
        )

    def in_window(block, shift):
        return lax.ppermute(
            block, "tile", [(i, i + shift) for i in range(tiles) if 0 <= i + shift < tiles]
        )

    def partner(block):
        return lax.ppermute(block, "tile", [(i, i ^ 1) for i in range(tiles)])

    def by_core(block, distance):
        route = [(i, (i + 2 * distance) % tiles) for i in range(0, tiles, 2)]
        route += [(i, (i - 2 * distance) % tiles) for i in range(1, tiles, 2)]
        return lax.ppermute(block, "tile", route)

    first = core == 0
    mine = jnp.where(first, text_key, text_value)
    other = partner(jnp.where(first, text_value, text_key))
    block = jnp.concatenate([jnp.where(first, mine, other), jnp.where(first, other, mine)], axis=0)

    key_below, key_above = in_window(self_key, 2), in_window(self_key, -2)
    value_below, value_above = in_window(self_value, 2), in_window(self_value, -2)
    key_partner, value_partner = partner(self_key), partner(self_value)

    block_below, block_above = from_chip(block, stride), from_chip(block, -stride)
    block_far = by_core(jnp.where(first, block_below, block_above), stride)
    gathered = jnp.concatenate([block, block_below, block_above, block_far], axis=0)
    lower, upper = [gathered], [gathered]
    for _ in range(stride // 2 - 1):
        lower.append(from_chip(lower[-1], 1))
        upper.append(from_chip(upper[-1], -1))
    last = by_core(jnp.where(first, lower[-1], upper[-1]), 1)
    pieces = [gathered, *lower[1:], *upper[1:], last]
    their_pieces = [partner(piece) for piece in pieces]

    key_next = partner(jnp.where(first, key_above, key_below))
    value_next = partner(jnp.where(first, value_above, value_below))
    step = jnp.where(first, -1, 1)
    position = jnp.stack([place - 2, place + 2, place + step])
    bias = jnp.where((position >= 0) & (position < tiles), 0.0, -1e30).astype(jnp.float32)
    gate_row = lax.dynamic_slice_in_dim(gate_table, timestep[0], 1, 0).astype(jnp.float32)
    self_part = self_attention(
        bias,
        gate_row,
        self_query,
        (self_key, key_partner, key_below, key_above, key_next),
        (self_value, value_partner, value_below, value_above, value_next),
    )
    return cross_attention(core[None], cross_query, self_part, pieces, their_pieces)


def solution(mesh):
    rows = P(("groups", "tile"), None)
    return jax.shard_map(
        shards,
        mesh=mesh,
        in_specs=(rows,) * 6 + (P(), P()),
        out_specs=rows,
        check_vma=False,
    )
```

```python
import math

import jax
import jax.numpy as jnp
from jax import lax
from jax.experimental import pallas as pl
from jax.experimental.pallas import tpu as pltpu
from jax.sharding import PartitionSpec as P

HEADS = 32
LOG2E = 1.4426950408889634
SELF_FEATURES = 1024
FEATURES = 1024
KEY_PARTS = 2
VALUE_PARTS = 2
CALLS = 2


def scores_of(queries, keys):
    return lax.dot_general(
        queries, keys, (((1,), (1,)), ((), ())), preferred_element_type=jnp.float32
    )


def self_kernel(bias_ref, step_ref, gate_ref, query_ref, *refs, head_dim):
    key_refs, value_refs, out_ref = refs[:5], refs[5:10], refs[-1]
    scale = LOG2E / math.sqrt(head_dim)
    rows = key_refs[0].shape[0]
    steps = lax.broadcasted_iota(jnp.int32, gate_ref.shape, 0)
    gates = jnp.where(steps == step_ref[0], gate_ref[...].astype(jnp.float32), 0.0)
    gates = jnp.sum(gates, axis=0, keepdims=True)
    for head in range(query_ref.shape[1] // head_dim):
        cols = slice(head * head_dim, (head + 1) * head_dim)
        keys = jnp.concatenate([ref[:, cols] for ref in key_refs], axis=0)
        values = jnp.concatenate([ref[:, cols] for ref in value_refs], axis=0)
        scores = scores_of(query_ref[:, cols], keys)
        scores = jnp.concatenate(
            [scores[:, : 2 * rows]]
            + [scores[:, k * rows : (k + 1) * rows] + bias_ref[k - 2] for k in range(2, 5)],
            axis=1,
        )
        top = jnp.max(scores, axis=1, keepdims=True) * scale
        weights = jnp.exp2(scores * scale - top)
        total = jnp.sum(weights, axis=1, keepdims=True)
        summed = jnp.dot(
            weights.astype(jnp.bfloat16), values, preferred_element_type=jnp.float32
        )
        out_ref[:, cols] = summed * (1.0 / total) * gates[:, cols]


def cross_kernel(core_ref, query_ref, self_ref, *refs, head_dim):
    mine, theirs, out_ref = refs[:8], refs[8:16], refs[16]
    key_buf, value_buf = refs[17], refs[18]
    rows = mine[0].shape[0]
    part = rows // 4

    def fill(keys, values):
        for k in range(8):
            key_buf[k * rows : (k + 1) * rows, :] = keys[k][...]
        for k in range(7):
            value_buf[k * rows : (k + 1) * rows, :] = values[k][...]
        for to, source in enumerate((1, 3, 0, 2)):
            first = 7 * rows + to * part
            value_buf[first : first + part, :] = values[7][source * part : (source + 1) * part, :]

    @pl.when(core_ref[0] == 0)
    def _():
        fill(mine, theirs)

    @pl.when(core_ref[0] != 0)
    def _():
        fill(theirs, mine)

    scale = LOG2E / math.sqrt(head_dim)
    for head in range(query_ref.shape[1] // head_dim):
        cols = slice(head * head_dim, (head + 1) * head_dim)
        scores = scores_of(query_ref[:, cols], key_buf[:, cols])
        top = jnp.max(scores, axis=1, keepdims=True) * scale
        weights = jnp.exp2(scores * scale - top)
        total = jnp.sum(weights, axis=1, keepdims=True)
        summed = jnp.dot(
            weights.astype(jnp.bfloat16), value_buf[:, cols], preferred_element_type=jnp.float32
        )
        out_ref[:, cols] = (self_ref[:, cols] + summed * (1.0 / total)).astype(out_ref.dtype)


def self_attention(bias, timestep, gates, queries, keys, values, first, width, partial):
    rows, whole = queries.shape
    features = min(SELF_FEATURES, width)
    offset = first // features

    def block_of(array):
        skip = first % array.shape[1] // features
        return pl.BlockSpec((array.shape[0], features), lambda i: (0, i + skip))

    arrays = (gates, queries, *keys, *values)
    in_specs = [pl.BlockSpec(memory_space=pltpu.SMEM)] * 2 + [block_of(array) for array in arrays]
    aliases = {}
    if partial is not None:
        aliases = {len(in_specs): 0}
        in_specs.append(pl.BlockSpec(memory_space=pl.ANY))
        arrays += (partial,)
    return pl.pallas_call(
        lambda *refs: self_kernel(*refs, head_dim=whole // HEADS),
        grid=(width // features,),
        in_specs=in_specs,
        out_specs=pl.BlockSpec((rows, features), lambda i: (0, i + offset)),
        out_shape=jax.ShapeDtypeStruct((rows, whole), jnp.float32),
        input_output_aliases=aliases,
        name="self_attention",
    )(bias, timestep, *arrays)


def cross_attention(core, queries, self_part, mine, theirs):
    rows, width = queries.shape
    text_rows = sum(piece.shape[0] for piece in mine)
    block = pl.BlockSpec((rows, FEATURES), lambda i: (0, i))
    piece_block = pl.BlockSpec((mine[0].shape[0], FEATURES), lambda i: (0, i))
    return pl.pallas_call(
        lambda *refs: cross_kernel(*refs, head_dim=width // HEADS),
        grid=(width // FEATURES,),
        in_specs=[pl.BlockSpec(memory_space=pltpu.SMEM), block, block] + [piece_block] * 16,
        out_specs=block,
        out_shape=jax.ShapeDtypeStruct((rows, width), queries.dtype),
        scratch_shapes=[pltpu.VMEM((text_rows, FEATURES), queries.dtype)] * 2,
        name="cross_attention",
    )(core, queries, self_part, *mine, *theirs)


def shards(
    self_query, self_key, self_value, cross_query, text_key, text_value, timestep, gate_table
):
    tiles = lax.axis_size("tile")
    chips = tiles // 2
    stride = chips // 4
    place = lax.axis_index("tile")
    core = place % 2
    width = self_query.shape[1]
    first = core == 0

    def send(block, route):
        return lax.ppermute(block, "tile", route)

    def from_chip(block, distance):
        return send(block, [(i, (i + 2 * distance) % tiles) for i in range(tiles)])

    def in_window(block, shift):
        return send(block, [(i, i + shift) for i in range(tiles) if 0 <= i + shift < tiles])

    def partner(block):
        return send(block, [(i, i ^ 1) for i in range(tiles)])

    def by_core(block, distance):
        route = [(i, (i + 2 * distance) % tiles) for i in range(0, tiles, 2)]
        route += [(i, (i - 2 * distance) % tiles) for i in range(1, tiles, 2)]
        return send(block, route)

    key_partner, value_partner = partner(self_key), partner(self_value)

    their_key, their_value = partner(text_key), partner(text_value)
    block = jnp.where(
        first,
        jnp.concatenate([text_key, their_key], axis=0),
        jnp.concatenate([their_value, text_value], axis=0),
    )
    block_below, block_above = from_chip(block, stride), from_chip(block, -stride)
    block_far = by_core(jnp.where(first, block_below, block_above), stride)
    gathered = jnp.concatenate([block, block_below, block_above, block_far], axis=0)
    lower, upper = [gathered], [gathered]
    for _ in range(1, stride // 2):
        lower.append(from_chip(lower[-1], 1))
        upper.append(from_chip(upper[-1], -1))
    last = by_core(jnp.where(first, lower[-1], upper[-1]), 1)
    pieces = [gathered, *lower[1:], *upper[1:], last]
    their_pieces = [partner(piece) for piece in pieces]

    step = jnp.where(first, -1, 1)
    position = jnp.stack([place - 2, place + 2, place + step])
    bias = jnp.where((position >= 0) & (position < tiles), 0.0, -1e30).astype(jnp.float32)

    def window_of(array, parts):
        span = width // parts
        pieces = []
        for part in range(parts):
            if part > 0:
                array, _ = lax.optimization_barrier((array, block_below))
            piece = lax.slice_in_dim(array, part * span, (part + 1) * span, axis=1)
            below = in_window(piece, 2)
            above = in_window(piece, -2)
            following = partner(jnp.where(first, above, below))
            pieces.append((below, above, following))
        return pieces

    keys = window_of(self_key, KEY_PARTS)
    values = window_of(self_value, VALUE_PARTS)
    self_part = None
    share = width // CALLS
    for call in range(CALLS):
        self_part = self_attention(
            bias,
            timestep,
            gate_table,
            self_query,
            (self_key, key_partner, *keys[call * KEY_PARTS // CALLS]),
            (self_value, value_partner, *values[call * VALUE_PARTS // CALLS]),
            call * share,
            share,
            self_part,
        )
    return cross_attention(core[None], cross_query, self_part, pieces, their_pieces)


def solution(mesh):
    rows = P(("groups", "tile"), None)
    return jax.shard_map(
        shards,
        mesh=mesh,
        in_specs=(rows,) * 6 + (P(), P()),
        out_specs=rows,
        check_vma=False,
    )
```

```python
import math

import jax
import jax.numpy as jnp
from jax import lax
from jax.experimental import pallas as pl
from jax.experimental.pallas import tpu as pltpu
from jax.sharding import PartitionSpec as P

HEADS = 32
LOG2E = 1.4426950408889634
SELF_FEATURES = 1024
FEATURES = 2048


def scores_of(queries, keys):
    return lax.dot_general(
        queries, keys, (((1,), (1,)), ((), ())), preferred_element_type=jnp.float32
    )


def self_kernel(bias_ref, step_ref, gate_ref, query_ref, *refs, head_dim):
    key_refs, value_refs, out_ref = refs[:5], refs[5:10], refs[-1]
    scale = LOG2E / math.sqrt(head_dim)
    rows = key_refs[0].shape[0]
    steps = lax.broadcasted_iota(jnp.int32, gate_ref.shape, 0)
    gates = jnp.where(steps == step_ref[0], gate_ref[...].astype(jnp.float32), 0.0)
    gates = jnp.sum(gates, axis=0, keepdims=True)

    def columns(refs, head):
        cols = slice(head * head_dim, (head + 1) * head_dim)
        return jnp.concatenate([ref[:, cols] for ref in refs], axis=0)

    heads = query_ref.shape[1] // head_dim
    ahead = scores_of(columns([query_ref], 0), columns(key_refs, 0))
    for head in range(heads):
        scores = ahead
        if head + 1 < heads:
            ahead = scores_of(columns([query_ref], head + 1), columns(key_refs, head + 1))
        cols = slice(head * head_dim, (head + 1) * head_dim)
        scores = jnp.concatenate(
            [scores[:, : 2 * rows]]
            + [scores[:, k * rows : (k + 1) * rows] + bias_ref[k - 2] for k in range(2, 5)],
            axis=1,
        )
        top = jnp.max(scores, axis=1, keepdims=True) * scale
        weights = jnp.exp2(scores * scale - top)
        total = jnp.sum(weights, axis=1, keepdims=True)
        summed = jnp.dot(
            weights.astype(jnp.bfloat16),
            columns(value_refs, head),
            preferred_element_type=jnp.float32,
        )
        out_ref[:, cols] = summed * (1.0 / total) * gates[:, cols]


def cross_kernel(core_ref, query_ref, self_ref, *refs, head_dim):
    mine, theirs, out_ref = refs[:8], refs[8:16], refs[16]
    key_buf, value_buf = refs[17], refs[18]
    rows = mine[0].shape[0]
    part = rows // 4

    def fill(keys, values):
        for k in range(8):
            key_buf[k * rows : (k + 1) * rows, :] = keys[k][...]
        for k in range(7):
            value_buf[k * rows : (k + 1) * rows, :] = values[k][...]
        for to, source in enumerate((1, 3, 0, 2)):
            first = 7 * rows + to * part
            value_buf[first : first + part, :] = values[7][source * part : (source + 1) * part, :]

    @pl.when(core_ref[0] == 0)
    def _():
        fill(mine, theirs)

    @pl.when(core_ref[0] != 0)
    def _():
        fill(theirs, mine)

    scale = LOG2E / math.sqrt(head_dim)
    heads = query_ref.shape[1] // head_dim
    ahead = scores_of(query_ref[:, :head_dim], key_buf[:, :head_dim])
    for head in range(heads):
        cols = slice(head * head_dim, (head + 1) * head_dim)
        scores = ahead
        if head + 1 < heads:
            after = slice((head + 1) * head_dim, (head + 2) * head_dim)
            ahead = scores_of(query_ref[:, after], key_buf[:, after])
        top = jnp.max(scores, axis=1, keepdims=True) * scale
        weights = jnp.exp2(scores * scale - top)
        total = jnp.sum(weights, axis=1, keepdims=True)
        summed = jnp.dot(
            weights.astype(jnp.bfloat16), value_buf[:, cols], preferred_element_type=jnp.float32
        )
        out_ref[:, cols] = (self_ref[:, cols] + summed * (1.0 / total)).astype(out_ref.dtype)


def self_attention(bias, timestep, gates, queries, keys, values, first, width, partial):
    rows, whole = queries.shape
    features = min(SELF_FEATURES, width // 2)
    offset = first // features

    def block_of(array):
        skip = offset if array.shape[1] == whole else 0
        return pl.BlockSpec((array.shape[0], features), lambda i: (0, i + skip))

    arrays = (gates, queries, *keys, *values)
    in_specs = [pl.BlockSpec(memory_space=pltpu.SMEM)] * 2 + [block_of(array) for array in arrays]
    aliases = {}
    if partial is not None:
        aliases = {len(in_specs): 0}
        in_specs.append(pl.BlockSpec(memory_space=pl.ANY))
        arrays += (partial,)
    return pl.pallas_call(
        lambda *refs: self_kernel(*refs, head_dim=whole // HEADS),
        grid=(width // features,),
        in_specs=in_specs,
        out_specs=pl.BlockSpec((rows, features), lambda i: (0, i + offset)),
        out_shape=jax.ShapeDtypeStruct((rows, whole), jnp.float32),
        input_output_aliases=aliases,
        name="self_attention",
    )(bias, timestep, *arrays)


def cross_attention(core, queries, self_part, mine, theirs):
    rows, width = queries.shape
    text_rows = sum(piece.shape[0] for piece in mine)
    block = pl.BlockSpec((rows, FEATURES), lambda i: (0, i))
    piece_block = pl.BlockSpec((mine[0].shape[0], FEATURES), lambda i: (0, i))
    return pl.pallas_call(
        lambda *refs: cross_kernel(*refs, head_dim=width // HEADS),
        grid=(width // FEATURES,),
        in_specs=[pl.BlockSpec(memory_space=pltpu.SMEM), block, block] + [piece_block] * 16,
        out_specs=block,
        out_shape=jax.ShapeDtypeStruct((rows, width), queries.dtype),
        scratch_shapes=[pltpu.VMEM((text_rows, FEATURES), queries.dtype)] * 2,
        name="cross_attention",
    )(core, queries, self_part, *mine, *theirs)


def shards(
    self_query, self_key, self_value, cross_query, text_key, text_value, timestep, gate_table
):
    tiles = lax.axis_size("tile")
    chips = tiles // 2
    stride = chips // 4
    place = lax.axis_index("tile")
    core = place % 2
    width = self_query.shape[1]
    first = core == 0

    def send(block, route):
        return lax.ppermute(block, "tile", route)

    def from_chip(block, distance):
        return send(block, [(i, (i + 2 * distance) % tiles) for i in range(tiles)])

    def in_window(block, shift):
        return send(block, [(i, i + shift) for i in range(tiles) if 0 <= i + shift < tiles])

    def partner(block):
        return send(block, [(i, i ^ 1) for i in range(tiles)])

    def by_core(block, distance):
        route = [(i, (i + 2 * distance) % tiles) for i in range(0, tiles, 2)]
        route += [(i, (i - 2 * distance) % tiles) for i in range(1, tiles, 2)]
        return send(block, route)

    key_partner, value_partner = partner(self_key), partner(self_value)

    their_key, their_value = partner(text_key), partner(text_value)
    block = jnp.where(
        first,
        jnp.concatenate([text_key, their_key], axis=0),
        jnp.concatenate([their_value, text_value], axis=0),
    )
    block_below, block_above = from_chip(block, stride), from_chip(block, -stride)
    block_far = by_core(jnp.where(first, block_below, block_above), stride)
    gathered = jnp.concatenate([block, block_below, block_above, block_far], axis=0)
    lower, upper = [gathered], [gathered]
    for _ in range(1, stride // 2):
        lower.append(from_chip(lower[-1], 1))
        upper.append(from_chip(upper[-1], -1))
    last = by_core(jnp.where(first, lower[-1], upper[-1]), 1)
    pieces = [gathered, *lower[1:], *upper[1:], last]
    their_pieces = [partner(piece) for piece in pieces]

    step = jnp.where(first, -1, 1)
    position = jnp.stack([place - 2, place + 2, place + step])
    bias = jnp.where((position >= 0) & (position < tiles), 0.0, -1e30).astype(jnp.float32)
    bounds = (0, width // 2, width)

    def window_of(array):
        pieces = []
        for part, (start, end) in enumerate(zip(bounds, bounds[1:])):
            if part > 0:
                array, _ = lax.optimization_barrier((array, block_below))
            piece = lax.slice_in_dim(array, start, end, axis=1)
            below = in_window(piece, 2)
            above = in_window(piece, -2)
            following = partner(jnp.where(first, above, below))
            pieces.append((below, above, following))
        return pieces

    keys = window_of(self_key)
    values = window_of(self_value)
    self_part = None
    for part, (start, end) in enumerate(zip(bounds, bounds[1:])):
        self_part = self_attention(
            bias,
            timestep,
            gate_table,
            self_query,
            (self_key, key_partner, *keys[part]),
            (self_value, value_partner, *values[part]),
            start,
            end - start,
            self_part,
        )
    return cross_attention(core[None], cross_query, self_part, pieces, their_pieces)


def solution(mesh):
    rows = P(("groups", "tile"), None)
    return jax.shard_map(
        shards,
        mesh=mesh,
        in_specs=(rows,) * 6 + (P(), P()),
        out_specs=rows,
        check_vma=False,
    )
```
